8 devices in a mesh: pair: 1 (over z), tp: 2 (over y), side: 4 (over x, core).
Axes of the slice: x: 2, y: 2, z: 1, core: 2. Of those that a mesh axis runs over, the one named last changes fastest.
Arguments:
- prompt_x: bfloat16 [6144, 2560], P(('pair', 'side'))
- s_len: int32 [4], P(('pair', 'side'))
- w_qkv_pre: bfloat16 [1, 2560, 3, 20, 128], P(None, None, None, 'tp')
- w_out_pre: bfloat16 [1, 20, 128, 2560], P(None, 'tp')
- w_gu_pre: bfloat16 [1, 2, 6912, 2560], P(None, None, 'tp')
- w_down_pre: bfloat16 [1, 6912, 2560], P(None, 'tp')
- gain_pre: float32 [1, 2, 2560], replicated
- dec_tokens: bfloat16 [128, 2560], P(('pair', 'side'))
- k_cache: bfloat16 [1, 128, 256, 10, 2, 128], P(None, ('pair', 'side'), None, None, 'tp')
- v_cache: bfloat16 [1, 128, 256, 10, 2, 128], P(None, ('pair', 'side'), None, None, 'tp')
- c_len: int32 [128], P(('pair', 'side'))
- w_qkv_dec: bfloat16 [1, 2560, 3, 10, 2, 128], P(None, None, None, None, 'tp')
- w_out_dec: bfloat16 [1, 10, 2, 128, 2560], P(None, None, 'tp')
- w_gu_dec: bfloat16 [1, 2, 6912, 2560], P(None, None, 'tp')
- w_down_dec: bfloat16 [1, 6912, 2560], P(None, 'tp')
- gain_dec: float32 [1, 2, 2560], replicated
Outputs:
- output 1: bfloat16 [6144, 2560], P(('pair', 'side'))
- output 2: bfloat16 [128, 2560], P(('pair', 'side'))
- output 3: bfloat16 [1, 6144, 10, 2, 128], P(None, ('pair', 'side'), None, 'tp')
- output 4: bfloat16 [1, 6144, 10, 2, 128], P(None, ('pair', 'side'), None, 'tp')
- output 5: bfloat16 [1, 128, 256, 10, 2, 128], P(None, ('pair', 'side'), None, None, 'tp')
- output 6: bfloat16 [1, 128, 256, 10, 2, 128], P(None, ('pair', 'side'), None, None, 'tp')
All inputs are finite; a program needn't handle non-finite values.
Results may differ from the reference program's by a relative error of at most 0.0126113.
Values are sent between devices in bfloat16 or wider.
A program may use at most 1 GiB of HBM per device.

```python
import jax
import jax.numpy as jnp
from jax import lax

D = 2560
HEADS = 20
HEAD = 128
FF = 6912
LAYERS = 1
PROMPT = 1536
BATCH = 32
CACHE = 256
TP_SIZE = 2
SIDES = 4

EPSILON = 1e-6
THETA = 10000.0
QK_GAIN = 1.5
OUT_GAIN = 2.0
MASKED = -1e30


def draw_int_inputs(len_key, cache_key):
    low_prompt = PROMPT // 2
    len_keys = jax.random.split(len_key, 2)
    s_len = jax.random.randint(len_keys[0], (SIDES,), low_prompt, PROMPT + 1, dtype=jnp.int32)
    slot_top = jax.random.randint(len_keys[1], (), 0, SIDES, dtype=jnp.int32)
    s_len = s_len.at[slot_top].set(PROMPT).at[(slot_top + 1) % SIDES].set(low_prompt)
    low_cache = CACHE // 4
    row_total = SIDES * BATCH
    cache_keys = jax.random.split(cache_key, 2)
    c_len = jax.random.randint(cache_keys[0], (row_total,), low_cache, CACHE, dtype=jnp.int32)
    row_top = jax.random.randint(cache_keys[1], (), 0, row_total, dtype=jnp.int32)
    c_len = c_len.at[row_top].set(CACHE - 1).at[(row_top + 1) % row_total].set(low_cache)
    return s_len, c_len


def draw_weights(weight_key):
    weight_keys = jax.random.split(weight_key, 5)
    qkv_scale = jnp.array([QK_GAIN, QK_GAIN, 1.0], jnp.float32)[:, None, None] * D ** -0.5
    w_qkv = (jax.random.normal(weight_keys[0], (LAYERS, D, 3, HEADS, HEAD), jnp.float32) * qkv_scale).astype(jnp.bfloat16)
    w_out = (jax.random.normal(weight_keys[1], (LAYERS, HEADS, HEAD, D), jnp.float32) * (OUT_GAIN * (HEADS * HEAD) ** -0.5)).astype(jnp.bfloat16)
    w_gu = (jax.random.normal(weight_keys[2], (LAYERS, 2, FF, D), jnp.float32) * D ** -0.5).astype(jnp.bfloat16)
    w_down = (jax.random.normal(weight_keys[3], (LAYERS, FF, D), jnp.float32) * FF ** -0.5).astype(jnp.bfloat16)
    gains = jax.random.uniform(weight_keys[4], (LAYERS, 2, D), jnp.float32, 0.5, 1.5)
    return w_qkv, w_out, w_gu, w_down, gains


def setup_inputs(seed: int = 0, part: int = 0) -> dict:
    shared_keys = jax.random.split(jax.random.key(seed + 1), 2)
    part_keys = jax.random.split(jax.random.fold_in(jax.random.key(seed), part), 6)
    heads_tp = HEADS // TP_SIZE
    w_qkv_pre, w_out_pre, w_gu_pre, w_down_pre, gain_pre = draw_weights(shared_keys[0])
    w_qkv_dec, w_out_dec, w_gu_dec, w_down_dec, gain_dec = draw_weights(shared_keys[1])
    s_len, c_len = draw_int_inputs(part_keys[0], part_keys[1])
    prompt_x = jax.random.normal(part_keys[2], (SIDES * PROMPT, D), jnp.float32).astype(jnp.bfloat16)
    dec_tokens = jax.random.normal(part_keys[3], (SIDES * BATCH, D), jnp.float32).astype(jnp.bfloat16)
    cache_shape = (LAYERS, SIDES * BATCH, CACHE, heads_tp, TP_SIZE, HEAD)
    k_cache = (jax.random.normal(part_keys[4], cache_shape, jnp.float32) * QK_GAIN).astype(jnp.bfloat16)
    v_cache = jax.random.normal(part_keys[5], cache_shape, jnp.float32).astype(jnp.bfloat16)
    return {'prompt_x': prompt_x, 's_len': s_len, 'w_qkv_pre': w_qkv_pre, 'w_out_pre': w_out_pre, 'w_gu_pre': w_gu_pre, 'w_down_pre': w_down_pre, 'gain_pre': gain_pre, 'dec_tokens': dec_tokens, 'k_cache': k_cache, 'v_cache': v_cache, 'c_len': c_len, 'w_qkv_dec': w_qkv_dec.reshape(LAYERS, D, 3, heads_tp, TP_SIZE, HEAD), 'w_out_dec': w_out_dec.reshape(LAYERS, heads_tp, TP_SIZE, HEAD, D), 'w_gu_dec': w_gu_dec, 'w_down_dec': w_down_dec, 'gain_dec': gain_dec}


def rms_norm(hidden, gain_vec):
    hid_f32 = hidden.astype(jnp.float32)
    inv_rms = lax.rsqrt(jnp.mean(hid_f32 * hid_f32, axis=-1, keepdims=True) + EPSILON)
    return (hid_f32 * inv_rms * gain_vec).astype(jnp.bfloat16)


def add_residual(hidden, update):
    return (hidden.astype(jnp.float32) + update.astype(jnp.float32)).astype(jnp.bfloat16)


def rope_tables(positions):
    half_dim = HEAD // 2
    inv_freq = THETA ** (-jnp.arange(half_dim, dtype=jnp.float32) * 2.0 / HEAD)
    angles = positions.astype(jnp.float32)[:, None] * inv_freq[None, :]
    return jnp.cos(angles), jnp.sin(angles)


def apply_rope(values_in, cos_tab, sin_tab):
    half_dim = values_in.shape[-1] // 2
    lower_half = values_in[..., :half_dim]
    upper_half = values_in[..., half_dim:]
    cos_b = cos_tab[:, None, :]
    sin_b = sin_tab[:, None, :]
    return jnp.concatenate([lower_half * cos_b - upper_half * sin_b, upper_half * cos_b + lower_half * sin_b], axis=-1)


def mlp_block(hidden, gain_vec, w_gu, w_down):
    normed = rms_norm(hidden, gain_vec)
    gate_up = jnp.einsum('sd,kfd->skf', normed.astype(jnp.float32), w_gu.astype(jnp.float32))
    gate_val = gate_up[:, 0].astype(jnp.bfloat16).astype(jnp.float32)
    up_val = gate_up[:, 1].astype(jnp.bfloat16).astype(jnp.float32)
    activated = (jax.nn.silu(gate_val) * up_val).astype(jnp.bfloat16)
    down_out = jnp.dot(activated, w_down, preferred_element_type=jnp.float32).astype(jnp.bfloat16)
    return add_residual(hidden, down_out)


def prefill_one(x_inst, s_valid, w_qkv, w_out, w_gu, w_down, gains):
    positions = jnp.arange(PROMPT)
    cos_tab, sin_tab = rope_tables(positions)
    allowed = (positions[None, :] <= positions[:, None]) & (positions[None, :] < s_valid)

    def head_attention(head_in):
        q_head, k_head, v_head = head_in
        scores = jnp.einsum('qe,ke->qk', q_head.astype(jnp.float32), k_head.astype(jnp.float32)) * HEAD ** -0.5
        scores = jnp.where(allowed, scores, MASKED)
        prob_bf = jax.nn.softmax(scores, axis=-1).astype(jnp.bfloat16)
        return jnp.einsum('qk,ke->qe', prob_bf.astype(jnp.float32), v_head.astype(jnp.float32)).astype(jnp.bfloat16)

    def layer_step(hidden, layer_in):
        wqkv_l, wout_l, wgu_l, wdown_l, gain_l = layer_in
        normed = rms_norm(hidden, gain_l[0])
        qkv_out = jnp.einsum('sd,dkhe->skhe', normed.astype(jnp.float32), wqkv_l.astype(jnp.float32))
        queries = apply_rope(qkv_out[:, 0], cos_tab, sin_tab).astype(jnp.bfloat16)
        keys_new = apply_rope(qkv_out[:, 1], cos_tab, sin_tab).astype(jnp.bfloat16)
        values_new = qkv_out[:, 2].astype(jnp.bfloat16)
        context = lax.map(head_attention, (queries.transpose(1, 0, 2), keys_new.transpose(1, 0, 2), values_new.transpose(1, 0, 2)))
        attn_out = jnp.einsum('hse,hed->sd', context.astype(jnp.float32), wout_l.astype(jnp.float32)).astype(jnp.bfloat16)
        hidden = add_residual(hidden, attn_out)
        hidden = mlp_block(hidden, gain_l[1], wgu_l, wdown_l)
        return hidden, (keys_new, values_new)

    return lax.scan(layer_step, x_inst, (w_qkv, w_out, w_gu, w_down, gains))


def decode_rows(tokens, k_cache, v_cache, c_len, w_qkv, w_out, w_gu, w_down, gains):
    row_total = tokens.shape[0]
    cos_tab, sin_tab = rope_tables(c_len)
    cache_pos = jnp.arange(CACHE)
    k_flat = k_cache.reshape(LAYERS, row_total, CACHE, HEADS, HEAD)
    v_flat = v_cache.reshape(LAYERS, row_total, CACHE, HEADS, HEAD)
    wqkv_flat = w_qkv.reshape(LAYERS, D, 3, HEADS, HEAD)
    wout_flat = w_out.reshape(LAYERS, HEADS, HEAD, D)
    write_at = (cache_pos[None, :] == c_len[:, None])[:, :, None, None]

    def row_attention(row_in):
        q_row, k_row, v_row, kc_row, vc_row, len_row = row_in
        cache_scores = jnp.einsum('he,the->ht', q_row.astype(jnp.float32), kc_row.astype(jnp.float32)) * HEAD ** -0.5
        cache_scores = jnp.where(cache_pos[None, :] < len_row, cache_scores, MASKED)
        self_score = jnp.sum(q_row.astype(jnp.float32) * k_row.astype(jnp.float32), axis=-1) * HEAD ** -0.5
        joint_scores = jnp.concatenate([cache_scores, self_score[:, None]], axis=1)
        prob_bf = jax.nn.softmax(joint_scores, axis=-1).astype(jnp.bfloat16).astype(jnp.float32)
        context = jnp.einsum('ht,the->he', prob_bf[:, :CACHE], vc_row.astype(jnp.float32)) + prob_bf[:, CACHE:] * v_row.astype(jnp.float32)
        return context.astype(jnp.bfloat16)

    def layer_step(hidden, layer_in):
        wqkv_l, wout_l, wgu_l, wdown_l, gain_l, kc_l, vc_l = layer_in
        normed = rms_norm(hidden, gain_l[0])
        qkv_out = jnp.einsum('bd,dkhe->bkhe', normed.astype(jnp.float32), wqkv_l.astype(jnp.float32))
        queries = apply_rope(qkv_out[:, 0], cos_tab, sin_tab).astype(jnp.bfloat16)
        k_tok = apply_rope(qkv_out[:, 1], cos_tab, sin_tab).astype(jnp.bfloat16)
        v_tok = qkv_out[:, 2].astype(jnp.bfloat16)
        context = lax.map(row_attention, (queries, k_tok, v_tok, kc_l, vc_l, c_len))
        attn_out = jnp.einsum('bhe,hed->bd', context.astype(jnp.float32), wout_l.astype(jnp.float32)).astype(jnp.bfloat16)
        hidden = add_residual(hidden, attn_out)
        hidden = mlp_block(hidden, gain_l[1], wgu_l, wdown_l)
        kc_next = jnp.where(write_at, k_tok[:, None], kc_l)
        vc_next = jnp.where(write_at, v_tok[:, None], vc_l)
        return hidden, (kc_next, vc_next)

    final_tokens, (kc_all, vc_all) = lax.scan(layer_step, tokens, (wqkv_flat, wout_flat, w_gu, w_down, gains, k_flat, v_flat))
    return final_tokens, kc_all.reshape(k_cache.shape), vc_all.reshape(v_cache.shape)


def reference(prompt_x, s_len, w_qkv_pre, w_out_pre, w_gu_pre, w_down_pre, gain_pre, dec_tokens, k_cache, v_cache, c_len, w_qkv_dec, w_out_dec, w_gu_dec, w_down_dec, gain_dec):
    prompts = prompt_x.reshape(SIDES, PROMPT, D)

    def run_instance(inst_in):
        x_inst, s_valid = inst_in
        final_hidden, (k_all, v_all) = prefill_one(x_inst, s_valid, w_qkv_pre, w_out_pre, w_gu_pre, w_down_pre, gain_pre)
        return final_hidden, k_all, v_all

    final_hidden, k_all, v_all = lax.map(run_instance, (prompts, s_len))
    half_sides = SIDES // 2
    prompt_shape = (LAYERS, SIDES * PROMPT, HEADS // TP_SIZE, TP_SIZE, HEAD)
    k_prompt = jnp.roll(k_all, half_sides, axis=0).transpose(1, 0, 2, 3, 4).reshape(prompt_shape)
    v_prompt = jnp.roll(v_all, half_sides, axis=0).transpose(1, 0, 2, 3, 4).reshape(prompt_shape)
    dec_out, k_cache_new, v_cache_new = decode_rows(dec_tokens, k_cache, v_cache, c_len, w_qkv_dec, w_out_dec, w_gu_dec, w_down_dec, gain_dec)
    return (final_hidden.reshape(SIDES * PROMPT, D), dec_out, k_prompt, v_prompt, k_cache_new, v_cache_new)
```

```python
import functools

import jax
import jax.numpy as jnp
from jax import lax
from jax.experimental import pallas as pl
from jax.experimental.pallas import tpu as pltpu
from jax.sharding import PartitionSpec as P

EPSILON = 1e-6
THETA = 10000.0
MASKED = -1e30
LOG2E = 1.4426950408889634


def rms_norm(hidden, gain_vec):
    hid_f32 = hidden.astype(jnp.float32)
    inv_rms = lax.rsqrt(jnp.mean(hid_f32 * hid_f32, axis=-1, keepdims=True) + EPSILON)
    return (hid_f32 * inv_rms * gain_vec).astype(jnp.bfloat16)


def add_residual(hidden, update):
    return (hidden.astype(jnp.float32) + update.astype(jnp.float32)).astype(jnp.bfloat16)


def rope_tables(positions, head_dim):
    half_dim = head_dim // 2
    inv_freq = THETA ** (-jnp.arange(half_dim, dtype=jnp.float32) * 2.0 / head_dim)
    angles = positions.astype(jnp.float32)[:, None] * inv_freq[None, :]
    return jnp.cos(angles), jnp.sin(angles)


def apply_rope(values_in, cos_tab, sin_tab):
    half_dim = values_in.shape[-1] // 2
    lower_half = values_in[..., :half_dim]
    upper_half = values_in[..., half_dim:]
    cos_b = cos_tab[:, None, :]
    sin_b = sin_tab[:, None, :]
    return jnp.concatenate([lower_half * cos_b - upper_half * sin_b, upper_half * cos_b + lower_half * sin_b], axis=-1)


def project_pair(n_ref, w_pair, o_ref, cos_ref, sin_ref, block_rows, rope_first, rope_second):
    rows = n_ref.shape[0]
    head_dim = w_pair.shape[1] // 2
    for start in range(0, rows, block_rows):
        at = pl.ds(start, block_rows)
        acc = jnp.dot(n_ref[at, :], w_pair, preferred_element_type=jnp.float32)
        for idx, rope in enumerate((rope_first, rope_second)):
            part = acc[:, idx * head_dim:(idx + 1) * head_dim]
            if rope:
                part = part * cos_ref[at, :] + pltpu.roll(part, head_dim // 2, 1) * sin_ref[at, :]
            o_ref[idx, at, :] = part.astype(o_ref.dtype)


def qkv_kernel(x_ref, g_ref, w_ref, cos_ref, sin_ref, o_ref, n_ref, *, block_rows):
    @pl.when(pl.program_id(0) == 0)
    def _():
        def norm_rows(i, carry):
            at = pl.ds(pl.multiple_of(i * 64, 64), 64)
            hid = x_ref[at, :].astype(jnp.float32)
            inv = lax.rsqrt(jnp.mean(hid * hid, axis=-1, keepdims=True) + EPSILON)
            n_ref[at, :] = (hid * inv * g_ref[...]).astype(n_ref.dtype)
            return carry
        lax.fori_loop(0, x_ref.shape[0] // 64, norm_rows, 0)

    w_pair = jnp.concatenate([w_ref[0], w_ref[1]], axis=1)
    project_pair(n_ref, w_pair, o_ref, cos_ref.at[0], sin_ref.at[0], block_rows, True, True)


def qkv_project(x, gain, w_heads, cos2, sin2, rope_heads):
    seq, width = x.shape
    heads, _, head_dim = w_heads.shape
    rope_steps = rope_heads // 2
    table_spec = pl.BlockSpec((1, seq, head_dim), lambda i: (i // rope_steps, 0, 0))
    return pl.pallas_call(
        functools.partial(qkv_kernel, block_rows=512),
        grid=(heads // 2,),
        in_specs=[
            pl.BlockSpec((seq, width), lambda i: (0, 0)),
            pl.BlockSpec((1, width), lambda i: (0, 0)),
            pl.BlockSpec((2, width, head_dim), lambda i: (i, 0, 0)),
            table_spec,
            table_spec,
        ],
        out_specs=[
            pl.BlockSpec((2, seq, head_dim), lambda i: (i, 0, 0)),
            pl.BlockSpec((seq, width), lambda i: (0, 0)),
        ],
        out_shape=[
            jax.ShapeDtypeStruct((heads, seq, head_dim), jnp.bfloat16),
            jax.ShapeDtypeStruct((seq, width), jnp.bfloat16),
        ],
        compiler_params=pltpu.CompilerParams(vmem_limit_bytes=56 * 2**20),
        cost_estimate=pl.CostEstimate(flops=2 * seq * width * heads * head_dim, bytes_accessed=2 * (heads * head_dim * (width + seq) + 2 * seq * width), transcendentals=0),
        name="qkv_project",
    )(x, gain, w_heads, cos2, sin2)


def kv_kernel(n_ref, w_ref, cos_ref, sin_ref, o_ref, *, block_rows):
    w_pair = jnp.concatenate([w_ref[0, 0], w_ref[1, 0]], axis=1)
    project_pair(n_ref, w_pair, o_ref.at[:, 0], cos_ref.at[0], sin_ref.at[0], block_rows, True, False)


def kv_project(n, w_kv, cos2, sin2):
    seq, width = n.shape
    _, heads, _, head_dim = w_kv.shape
    table_spec = pl.BlockSpec((1, seq, head_dim), lambda i: (0, 0, 0))
    return pl.pallas_call(
        functools.partial(kv_kernel, block_rows=512),
        grid=(heads,),
        in_specs=[
            pl.BlockSpec((seq, width), lambda i: (0, 0)),
            pl.BlockSpec((2, 1, width, head_dim), lambda i: (0, i, 0, 0)),
            table_spec,
            table_spec,
        ],
        out_specs=pl.BlockSpec((2, 1, seq, head_dim), lambda i: (0, i, 0, 0)),
        out_shape=jax.ShapeDtypeStruct((2, heads, seq, head_dim), jnp.bfloat16),
        compiler_params=pltpu.CompilerParams(vmem_limit_bytes=48 * 2**20),
        cost_estimate=pl.CostEstimate(flops=4 * seq * width * heads * head_dim, bytes_accessed=2 * (2 * heads * head_dim * (width + seq) + seq * width), transcendentals=0),
        name="kv_project",
    )(n, w_kv, cos2, sin2)


def attention_kernel(len_ref, q_ref, k_ref, v_ref, o_ref, *, row_start, sub_rows, len_floor):
    heads_blk, rows, head_dim = q_ref.shape
    s_valid = len_ref[0]
    scale = head_dim ** -0.5 * LOG2E
    for head in range(heads_blk):
        for sub in range(0, rows, sub_rows):
            first = row_start + sub
            query = q_ref[head, pl.ds(sub, sub_rows), :]
            pieces = []
            if first > 0:
                part = lax.dot_general(query, k_ref[head, pl.ds(0, first), :], (((1,), (1,)), ((), ())), preferred_element_type=jnp.float32)
                if first > len_floor:
                    cols = lax.broadcasted_iota(jnp.int32, (1, first), 1)
                    part = jnp.where(cols < s_valid, part, MASKED)
                pieces.append((part, 0, first))
            part = lax.dot_general(query, k_ref[head, pl.ds(first, sub_rows), :], (((1,), (1,)), ((), ())), preferred_element_type=jnp.float32)
            row_ids = lax.broadcasted_iota(jnp.int32, (sub_rows, sub_rows), 0)
            col_ids = lax.broadcasted_iota(jnp.int32, (sub_rows, sub_rows), 1)
            part = jnp.where((col_ids <= row_ids) & (col_ids < s_valid - first), part, MASKED)
            pieces.append((part, first, sub_rows))
            top = functools.reduce(jnp.maximum, [jnp.max(p, axis=-1, keepdims=True) for p, _, _ in pieces])
            exps = [jnp.exp2((p - top) * scale) for p, _, _ in pieces]
            total = functools.reduce(jnp.add, [jnp.sum(e, axis=-1, keepdims=True) for e in exps])
            inv = 1.0 / total
            out = None
            for e, (_, start, size) in zip(exps, pieces):
                prob = (e * inv).astype(jnp.bfloat16)
                term = jnp.dot(prob, v_ref[head, pl.ds(start, size), :], preferred_element_type=jnp.float32)
                out = term if out is None else out + term
            o_ref[pl.ds(sub, sub_rows), pl.ds(head * head_dim, head_dim)] = out.astype(o_ref.dtype)


def attention_rows(s_valid, qkv, heads, row_start, rows):
    _, seq, head_dim = qkv.shape
    keys = row_start + rows
    blk = 2
    steps = heads // blk
    flops = 4 * rows * (row_start + rows // 2) * head_dim * heads
    return pl.pallas_call(
        functools.partial(attention_kernel, row_start=row_start, sub_rows=256, len_floor=seq // 2),
        grid_spec=pltpu.PrefetchScalarGridSpec(
            num_scalar_prefetch=1,
            grid=(steps,),
            in_specs=[
                pl.BlockSpec((blk, rows, head_dim), lambda i, s: (i, row_start // rows, 0)),
                pl.BlockSpec((blk, keys, head_dim), lambda i, s: (steps + i, 0, 0)),
                pl.BlockSpec((blk, keys, head_dim), lambda i, s: (2 * steps + i, 0, 0)),
            ],
            out_specs=pl.BlockSpec((rows, blk * head_dim), lambda i, s: (0, i)),
        ),
        out_shape=jax.ShapeDtypeStruct((rows, heads * head_dim), jnp.bfloat16),
        compiler_params=pltpu.CompilerParams(vmem_limit_bytes=48 * 2**20),
        cost_estimate=pl.CostEstimate(flops=4 * flops, bytes_accessed=2 * heads * head_dim * (2 * rows + 2 * keys), transcendentals=rows * keys * heads),
        name=f"attention_{row_start}",
    )(s_valid, qkv, qkv, qkv)


def decode_attention(queries, k_tok, v_tok, k_layer, v_layer, visible):
    attn_scale = queries.shape[-1] ** -0.5
    cache_scores = jnp.einsum('bhe,bthe->bht', queries, k_layer, preferred_element_type=jnp.float32) * attn_scale
    cache_scores = jnp.where(visible, cache_scores, MASKED)
    self_score = jnp.einsum('bhe,bhe->bh', queries, k_tok, preferred_element_type=jnp.float32) * attn_scale
    row_max = jnp.maximum(jnp.max(cache_scores, axis=-1), self_score)
    cache_exp = jnp.exp(cache_scores - row_max[..., None])
    self_exp = jnp.exp(self_score - row_max)
    denominator = jnp.sum(cache_exp, axis=-1) + self_exp
    cache_prob = (cache_exp / denominator[..., None]).astype(jnp.bfloat16)
    self_prob = (self_exp / denominator).astype(jnp.bfloat16).astype(jnp.float32)
    context = jnp.einsum('bht,bthe->bhe', cache_prob, v_layer, preferred_element_type=jnp.float32) + self_prob[..., None] * v_tok.astype(jnp.float32)
    return context.astype(jnp.bfloat16)


def swiglu(normed, w_gu, w_down):
    gate_up = jnp.einsum('sd,kfd->skf', normed, w_gu, preferred_element_type=jnp.float32)
    gate_val = gate_up[:, 0, :].astype(jnp.bfloat16).astype(jnp.float32)
    up_val = gate_up[:, 1, :].astype(jnp.bfloat16).astype(jnp.float32)
    activated = (jax.nn.silu(gate_val) * up_val).astype(jnp.bfloat16)
    return jnp.dot(activated, w_down, preferred_element_type=jnp.float32)


def run_decode(tokens, k_cache, v_cache, c_len, w_qkv, w_out, w_gu, w_down, gains, tp_sum):
    _, row_count, cache_len, heads_loc, _, head_dim = k_cache.shape
    width = tokens.shape[1]
    k_local = k_cache.reshape(row_count, cache_len, heads_loc, head_dim)
    v_local = v_cache.reshape(row_count, cache_len, heads_loc, head_dim)
    wqkv_local = w_qkv.reshape(width, 3, heads_loc, head_dim)
    wout_local = w_out.reshape(heads_loc, head_dim, width)
    cos_tab, sin_tab = rope_tables(c_len, head_dim)
    cache_pos = jnp.arange(cache_len)
    visible = (cache_pos[None, :] < c_len[:, None])[:, None, :]
    write_at = (cache_pos[None, :] == c_len[:, None])[:, :, None, None]
    normed = rms_norm(tokens, gains[0, 0])
    qkv_out = jnp.einsum('bd,dkhe->bkhe', normed, wqkv_local, preferred_element_type=jnp.float32)
    queries = apply_rope(qkv_out[:, 0], cos_tab, sin_tab).astype(jnp.bfloat16)
    k_tok = apply_rope(qkv_out[:, 1], cos_tab, sin_tab).astype(jnp.bfloat16)
    v_tok = qkv_out[:, 2].astype(jnp.bfloat16)
    context = decode_attention(queries, k_tok, v_tok, k_local, v_local, visible)
    part_sum = jnp.einsum('bhe,hed->bd', context, wout_local, preferred_element_type=jnp.float32)
    tokens = add_residual(tokens, tp_sum(part_sum).astype(jnp.bfloat16))
    mlp_part = swiglu(rms_norm(tokens, gains[0, 1]), w_gu[0], w_down[0])
    tokens = add_residual(tokens, tp_sum(mlp_part).astype(jnp.bfloat16))
    k_next = jnp.where(write_at, k_tok[:, None], k_local)
    v_next = jnp.where(write_at, v_tok[:, None], v_local)
    return tokens, k_next.reshape(k_cache.shape), v_next.reshape(v_cache.shape)


def solution(mesh):
    side_size = mesh.shape['side']
    half_sides = side_size // 2
    swap_tp = [(0, 1), (1, 0)]
    swap_x = [(idx, (idx + half_sides) % side_size) for idx in range(side_size)]
    swap_core = [(idx, idx ^ 1) for idx in range(side_size)]
    inst_axes = ('pair', 'side')
    rows_spec = P(inst_axes, None)
    vec_spec = P(inst_axes)
    cache_spec = P(None, inst_axes, None, None, 'tp', None)
    prompt_spec = P(None, inst_axes, None, 'tp', None)
    in_specs = (rows_spec, vec_spec, P(None, None, None, 'tp', None), P(None, 'tp', None, None), P(None, None, 'tp', None), P(None, 'tp', None), P(None, None, None), rows_spec, cache_spec, cache_spec, vec_spec, P(None, None, None, None, 'tp', None), P(None, None, 'tp', None, None), P(None, None, 'tp', None), P(None, 'tp', None), P(None, None, None))
    out_specs = (rows_spec, rows_spec, prompt_spec, prompt_spec, cache_spec, cache_spec)

    def device_fn(prompt_x, s_len, w_qkv_pre, w_out_pre, w_gu_pre, w_down_pre, gain_pre, dec_tokens, k_cache, v_cache, c_len, w_qkv_dec, w_out_dec, w_gu_dec, w_down_dec, gain_dec):
        seq, width = prompt_x.shape
        heads, head_dim = w_out_pre.shape[1], w_out_pre.shape[2]
        me_tp = lax.axis_index('tp')
        me_side = lax.axis_index('side')
        me_x, me_core = me_side // 2, me_side % 2
        quarter = me_core * 2 + me_x

        def to_tp(value):
            return lax.ppermute(value, 'tp', swap_tp)

        def tp_sum(value):
            return value + to_tp(value)

        def in_order(flag, mine, other, axis):
            return jnp.where(flag == 0, jnp.concatenate([mine, other], axis), jnp.concatenate([other, mine], axis))

        def fetch_partner(piece, axis):
            size = piece.shape[axis] // 4
            mine = lax.dynamic_slice_in_dim(piece, quarter * size, size, axis)
            got = to_tp(mine)
            got = in_order(me_x, got, lax.ppermute(got, 'side', swap_x), axis)
            return in_order(me_core, got, lax.ppermute(got, 'side', swap_core), axis)

        w_heads = w_qkv_pre[0].transpose(1, 2, 0, 3)
        w_out_own = w_out_pre[0].reshape(heads * head_dim, width)
        w_out_other = fetch_partner(w_out_own, 0)
        by_parity = w_heads[1:].reshape(2, heads // 2, 2, width, head_dim)
        w_kv_send = lax.dynamic_index_in_dim(by_parity, 1 - me_tp, 2, keepdims=False)
        w_kv_other = fetch_partner(w_kv_send, 2)

        cos_tab, sin_tab = rope_tables(jnp.arange(seq), head_dim)
        cos2 = jnp.stack([jnp.concatenate([cos_tab, cos_tab], 1), jnp.ones((seq, head_dim), jnp.float32)])
        sin2 = jnp.stack([jnp.concatenate([-sin_tab, sin_tab], 1), jnp.zeros((seq, head_dim), jnp.float32)])
        qkv, normed = qkv_project(prompt_x, gain_pre[0, 0:1], w_heads.reshape(3 * heads, width, head_dim), cos2, sin2, 2 * heads)

        kv_own = lax.dynamic_index_in_dim(qkv[heads:].reshape(2, heads // 2, 2, seq, head_dim), me_tp, 2, keepdims=False)
        kv_own = lax.ppermute(kv_own, 'side', swap_x)
        kv_more = lax.ppermute(kv_project(normed, w_kv_other, cos2, sin2), 'side', swap_x)
        prompt_kv = in_order(me_tp, kv_own, kv_more, 1)
        prompt_kv = prompt_kv.transpose(0, 2, 1, 3).reshape(2, 1, seq, heads, 1, head_dim)

        rows = seq // 3
        half = rows // 2
        w_out_all = jnp.concatenate([w_out_own, w_out_other], 0)
        hidden_out = jnp.zeros((seq, width), jnp.bfloat16)
        contexts = []
        for start in range(0, seq, rows):
            context = attention_rows(s_len, qkv, heads, start, rows)
            contexts.append(jnp.concatenate([context, to_tp(context)], 1))
        for idx, start in enumerate(range(0, seq, rows)):
            attn_out = jnp.dot(contexts[idx], w_out_all, preferred_element_type=jnp.float32).astype(jnp.bfloat16)
            hidden = add_residual(prompt_x[start:start + rows], attn_out)
            part = swiglu(rms_norm(hidden, gain_pre[0, 1]), w_gu_pre[0], w_down_pre[0])
            received = to_tp(lax.dynamic_slice_in_dim(part, (1 - me_tp) * half, half, 0))
            total = lax.dynamic_slice_in_dim(part, me_tp * half, half, 0) + received
            mine = add_residual(lax.dynamic_slice_in_dim(hidden, me_tp * half, half, 0), total.astype(jnp.bfloat16))
            hidden_out = lax.dynamic_update_slice_in_dim(hidden_out, mine, start + me_tp * half, 0)
            hidden_out = lax.dynamic_update_slice_in_dim(hidden_out, to_tp(mine), start + (1 - me_tp) * half, 0)

        dec_out, k_cache_new, v_cache_new = run_decode(dec_tokens, k_cache, v_cache, c_len, w_qkv_dec, w_out_dec, w_gu_dec, w_down_dec, gain_dec, tp_sum)
        return hidden_out, dec_out, prompt_kv[0], prompt_kv[1], k_cache_new, v_cache_new

    return jax.shard_map(device_fn, mesh=mesh, in_specs=in_specs, out_specs=out_specs, check_vma=False)
```
